32 devices in a mesh: ep: 16 (over z, y, x), tp: 2 (over core).
Axes of the slice: x: 2, y: 2, z: 4, core: 2. Of those that a mesh axis runs over, the one named last changes fastest.
Arguments:
- tokens: bfloat16 [2048, 3584], P('ep', 'tp'), may hold values from -6 to 6
- routes: int32 [2048, 8], P('ep'), may hold values from 0 to 15, all different within a row; in each aligned block of 128 rows (0 to 127, 128 to 255, ...) at most 72 rows name the same one
- gate_levels: int32 [2048, 8], P('ep'), may hold values from 1 to 255
- w_gate: bfloat16 [16, 3584, 1024], P('ep', 'tp'), may hold values from -0.09375 to 0.09375
- w_up: bfloat16 [16, 3584, 1024], P('ep', 'tp'), may hold values from -0.09375 to 0.09375
- w_down: bfloat16 [16, 1024, 3584], P('ep', None, 'tp'), may hold values from -0.1875 to 0.1875
Outputs:
- mixed: bfloat16 [2048, 3584], P('ep', 'tp')
The draws below stay inside these ranges and needn't reach their ends.
Inputs may be any that keep to these rules, and one draw needn't show every extreme that they name: `routes`: each row names 8 different experts. Among the 128 tokens of one aligned block no expert is named by more than 72 rows, and in every draw some expert is named by exactly 72 rows of some block.
All inputs are finite; a program needn't handle non-finite values.
Results may differ from the reference program's by a relative error of at most 0.0085.
Values may be sent and summed in bfloat16 or wider, within the bound.
A program may use at most 64 MiB of HBM per device.

```python
import math
import jax
import jax.numpy as jnp
import numpy as np
from jax import lax

D = 3584
FF = 1024
TOP = 8
TOK_EP = 128
EXPERTS = 16
CAP = 72
TOKENS = 2048
N_EP = 16


def plant(values, rng, least, largest):
    index_at = [jax.random.randint(jax.random.fold_in(rng, axis), (), 0, length) for axis, length in enumerate(values.shape)]
    main_axis = values.shape.index(max(values.shape))
    beside = index_at[:main_axis] + [(index_at[main_axis] + 1) % values.shape[main_axis]] + index_at[main_axis + 1:]
    return values.at[tuple(index_at)].set(least).at[tuple(beside)].set(largest)


def level_of(stream_key, extent, pieces, least, high):
    gain = 1.0
    for position, parts in pieces:
        draws = jax.random.uniform(jax.random.fold_in(jax.random.fold_in(stream_key, 6), position), (parts,), jnp.float32, least / len(pieces), high / len(pieces))
        gain = gain * jnp.repeat(jnp.exp(draws), extent[position] // parts).reshape((-1,) + (1,) * (len(extent) - 1 - position))
    return gain


def deal_out(rng, own, number, rows, count, top, bound, slope):
    order = jax.random.permutation(rng, count)
    packed, common = portions_of(count, rows * top, bound, slope, True), portions_of(count, rows * top, bound, slope, False)
    places = jnp.arange(count)

    def named(tallies, rotation):
        used = int((tallies > 0).sum())
        fixed = max(1, used // 4)
        passed = fixed + (places - fixed + rotation * (used - fixed)) % max(1, count - fixed)
        return jnp.zeros((count,), jnp.int32).at[order[jnp.where(places < fixed, places, passed)]].set(jnp.asarray(tallies, jnp.int32))

    tallies = jnp.where(number % 4 == 0, named(packed, number // 4), named(common, number - number // 4 - 1))
    mixed = jax.random.permutation(jax.random.fold_in(own, 3), count)
    giver, taker = mixed[0:count // 2 * 2:2], mixed[1:count // 2 * 2:2]
    room = jnp.minimum(tallies[giver] - 1, bound - tallies[taker]) // 2
    room = jnp.where((giver == order[0]) | (taker == order[0]) | (tallies[taker] == 0), 0, jnp.maximum(room, 0))
    passed = jax.random.randint(jax.random.fold_in(own, 4), (count // 2,), 0, 1 << 20) % (room + 1)
    tallies = tallies.at[giver].add(-passed).at[taker].add(passed)
    labels = jnp.searchsorted(jnp.cumsum(tallies), jnp.arange(rows * top), side="right").astype(jnp.int32)
    listing = labels.reshape(top, rows).T
    listing = listing[jax.random.permutation(jax.random.fold_in(own, 1), rows)]
    rotation = jax.random.randint(jax.random.fold_in(own, 2), (rows, 1), 0, top)
    return jnp.take_along_axis(listing, (jnp.arange(top)[None, :] + rotation) % top, axis=1)


def portions_of(count, total, limit, skew, full):
    portions = [(1 << 20) // math.isqrt(grade ** skew) + 1 for grade in range(1, count + 1)]
    largest = limit if full else min(limit, max(-(-total // count), total * portions[0] // sum(portions)))
    least = 1 if total - largest >= count - 1 else 0
    counts, rest = [largest] + [least] * (count - 1), total - largest - least * (count - 1)
    while rest > 0:
        movable = [i for i in range(1, count) if counts[i] < largest] or [i for i in range(1, count) if counts[i] < limit]
        mass, left = sum([portions[i] for i in movable]), rest
        for i in movable:
            more = min(limit - counts[i], max(1, left * portions[i] // mass), rest)
            counts[i] = counts[i] + more
            rest = rest - more
    return np.array(counts)


def gaussian(key, extent, deviation, reach, cuts=(), kind=jnp.bfloat16):
    loudness = level_of(key, extent, cuts, -0.22, 0.18) if cuts else 1.0
    entries = jax.random.normal(key, extent, jnp.float32) * deviation * loudness
    return jnp.minimum(jnp.maximum(entries, -reach), reach).astype(kind)


def setup_inputs(seed: int = 0) -> dict:
    arg_keys = jax.random.split(jax.random.key(seed), 7)
    tokens = gaussian(arg_keys[0], (TOKENS, D), 1.0, 6.0, ((0, 16), (1, 2)))
    routes_keys = jax.random.split(jax.random.fold_in(arg_keys[1], 1), TOKENS // TOK_EP)
    routes_turns = jax.random.permutation(jax.random.fold_in(arg_keys[1], 3), TOKENS // TOK_EP)
    routes = jax.vmap(lambda own, number: deal_out(jax.random.fold_in(arg_keys[1], 2), own, number, TOK_EP, EXPERTS, TOP, CAP, 2))(routes_keys, routes_turns).reshape((TOKENS, TOP))
    gate_levels = plant(jax.random.randint(arg_keys[2], (TOKENS, TOP), 1, 256), jax.random.fold_in(arg_keys[2], 1), 1, 255).astype(jnp.int32)
    w_gate = gaussian(arg_keys[3], (EXPERTS, D, FF), D ** -0.5, 0.09375, ((0, 16), (1, 2)))
    w_up = gaussian(arg_keys[4], (EXPERTS, D, FF), D ** -0.5, 0.09375, ((0, 16), (1, 2)))
    w_down = gaussian(arg_keys[5], (EXPERTS, FF, D), FF ** -0.5, 0.1875, ((0, 16), (2, 2)))
    return {"tokens": tokens, "routes": routes, "gate_levels": gate_levels, "w_gate": w_gate, "w_up": w_up, "w_down": w_down}


def expert_apply(operands):
    inputs, gate_w, up_w, down_w = operands
    gate_act = jnp.dot(inputs, gate_w, preferred_element_type=jnp.float32)
    up_act = jnp.dot(inputs, up_w, preferred_element_type=jnp.float32)
    hidden = (jax.nn.silu(gate_act) * up_act).astype(jnp.bfloat16)
    return jnp.dot(hidden, down_w, preferred_element_type=jnp.float32).astype(jnp.bfloat16)


def reference(tokens, routes, gate_levels, w_gate, w_up, w_down):
    block_rows = TOK_EP * TOP
    flat_ids = routes.reshape(N_EP, block_rows).astype(jnp.int32)
    same_expert = flat_ids[:, :, None] == flat_ids[:, None, :]
    positions = jnp.arange(block_rows, dtype=jnp.int32)
    earlier = positions[:, None] > positions[None, :]
    slot_index = jnp.sum(same_expert & earlier[None], axis=2).astype(jnp.int32)
    block_ids = jnp.arange(N_EP, dtype=jnp.int32)[:, None]
    buffer_index = (flat_ids * (N_EP * CAP) + block_ids * CAP + slot_index).reshape(-1).astype(jnp.int32)
    owners = (jnp.arange(TOKENS * TOP, dtype=jnp.int32) // TOP).astype(jnp.int32)
    expert_rows = jnp.zeros((EXPERTS * N_EP * CAP, D), jnp.bfloat16).at[buffer_index].set(tokens[owners])
    expert_rows = expert_rows.reshape(EXPERTS, N_EP * CAP, D)
    expert_out = lax.map(expert_apply, (expert_rows, w_gate, w_up, w_down))
    picked = expert_out.reshape(EXPERTS * N_EP * CAP, D)[buffer_index].reshape(TOKENS, TOP, D).astype(jnp.float32)
    levels = gate_levels.astype(jnp.float32)
    weights = levels / jnp.sum(levels, axis=1, keepdims=True)
    return jnp.sum(weights[:, :, None] * picked, axis=1).astype(jnp.bfloat16)
```

```python
import functools
import math

import jax
import jax.numpy as jnp
from jax import lax
from jax.experimental import pallas as pl
from jax.experimental.pallas import tpu as pltpu
from jax.sharding import PartitionSpec as P

MESH = pl.DeviceIdType.MESH
ABSENT = -65536.0
F32 = jnp.float32
BF16 = jnp.bfloat16


def run_expert(inputs, gate_w, up_w, down_w):
    gate_part = jnp.dot(inputs, gate_w, preferred_element_type=jnp.float32)
    up_part = jnp.dot(inputs, up_w, preferred_element_type=jnp.float32)
    gate_sum, up_sum = (
        lax.psum_scatter(gate_part, "tp", scatter_dimension=1, tiled=True),
        lax.psum_scatter(up_part, "tp", scatter_dimension=1, tiled=True),
    )
    hidden = (jax.nn.silu(gate_sum) * up_sum).astype(jnp.bfloat16)
    output = jnp.dot(
        lax.all_gather(hidden, "tp", axis=1, tiled=True), down_w, preferred_element_type=jnp.float32
    )
    return output.astype(jnp.bfloat16)


def general_path(tokens, routes, gate_levels, w_gate, w_up, w_down):
    ep_count = lax.axis_size("ep")
    tok_rows, top_count = routes.shape
    experts_here = w_gate.shape[0]
    capacity = capacity_of(tok_rows, top_count, experts_here * ep_count)
    width_local = tokens.shape[1]
    slots_each = ep_count * capacity
    slots_total = experts_here * slots_each
    flat_ids = routes.reshape(-1)
    positions = jnp.arange(tok_rows * top_count, dtype=jnp.int32)
    same_expert = flat_ids[:, None] == flat_ids[None, :]
    earlier = positions[:, None] > positions[None, :]
    slot_index = jnp.sum(same_expert & earlier, axis=1)
    destination = (
        flat_ids % experts_here * ep_count + flat_ids // experts_here
    ) * capacity + slot_index
    slot_numbers = jnp.arange(slots_total, dtype=jnp.int32)
    matches = destination.reshape(tok_rows, top_count)[:, :, None] == slot_numbers[None, None, :]
    token_slots = jnp.any(matches, axis=1).astype(jnp.bfloat16)
    outgoing = jnp.einsum(
        "ts,td->sd", token_slots, tokens, preferred_element_type=jnp.float32
    ).astype(jnp.bfloat16)
    levels = gate_levels.astype(jnp.float32)
    weights = levels / jnp.sum(levels, axis=1, keepdims=True)
    weight_high = weights.astype(jnp.bfloat16).astype(jnp.float32)
    weight_low = weights - weight_high
    table_high = jnp.sum(jnp.where(matches, weight_high[:, :, None], 0.0), axis=1).astype(
        jnp.bfloat16
    )
    table_low = jnp.sum(jnp.where(matches, weight_low[:, :, None], 0.0), axis=1).astype(
        jnp.bfloat16
    )
    arrived = lax.all_to_all(
        outgoing.reshape(experts_here, ep_count, capacity, width_local),
        "ep",
        split_axis=1,
        concat_axis=1,
        tiled=True,
    )
    expert_rows = arrived.reshape(experts_here, slots_each, width_local)
    results = [run_expert(expert_rows[0], w_gate[0], w_up[0], w_down[0])]
    produced = jnp.stack(results)
    returned = lax.all_to_all(
        produced.reshape(experts_here, ep_count, capacity, width_local),
        "ep",
        split_axis=1,
        concat_axis=1,
        tiled=True,
    )
    flat_returned = returned.reshape(slots_total, width_local)
    mixed = jnp.dot(table_high, flat_returned, preferred_element_type=jnp.float32)
    mixed = mixed + jnp.dot(table_low, flat_returned, preferred_element_type=jnp.float32)
    return mixed.astype(jnp.bfloat16)


def capacity_of(tok_rows, top_count, experts):
    return min(tok_rows, max(2, 9 * tok_rows * top_count // (8 * experts)))


def layer_kernel(
    line, plane, cap, fc,
    code_ref, levels_ref, tokens_hbm, wg_hbm, wu_hbm, wd_hbm, out_ref,
    tok, tbl_out, tbl, pick, mix, send, rows, rows_x, w_own, w_x, wd, acc, hid,
    outs, ret, part_f, part, zin, own,
    tok_sem, w_sem, wd_sem, ts_sem, tr_sem, zs_sem, zr_sem, ps_sem, pr_sem,
    xs_sem, xr_sem, ws_sem, wr_sem, hs_sem, hr_sem, bs_sem, br_sem, cs_sem, cr_sem,
):
    me = lax.axis_index("ep")
    t = lax.axis_index("tp")
    other = 1 - t
    z, p = me // plane, me % plane
    T, top = levels_ref.shape
    R = line * cap
    nc = tok.shape[0]
    half = wg_hbm.shape[1] // 2

    def z_at(d):
        return lax.rem(z + d, line)

    def p_at(k):
        return lax.rem(p + k, plane)

    def z_dev(d):
        return {"ep": z_at(d) * plane + p}

    def p_dev(k):
        return {"ep": z * plane + p_at(k)}

    def remote(src, dst, s, r, dev):
        return pltpu.make_async_remote_copy(
            src_ref=src, dst_ref=dst, send_sem=s, recv_sem=r, device_id=dev, device_id_type=MESH
        )

    def zrows(i):
        return pl.ds(pl.multiple_of(i * T, T), T)

    def prows(i):
        return pl.ds(pl.multiple_of(i * R, 16), R)

    def units(i):
        return pl.ds(pl.multiple_of(i * half, 128), half)

    def tok_load(c):
        return pltpu.make_async_copy(
            tokens_hbm.at[:, pl.ds(pl.multiple_of(c * fc, 128), fc)],
            tok.at[c, zrows(z)], tok_sem.at[c],
        )

    def wd_load(c):
        return pltpu.make_async_copy(
            wd_hbm.at[:, pl.ds(pl.multiple_of(c * fc, 128), fc)], wd.at[c], wd_sem.at[c]
        )

    def w_load(i):
        return pltpu.make_async_copy(
            (wg_hbm, wu_hbm)[i].at[:, units(t)], w_own.at[:, i * half:(i + 1) * half], w_sem.at[i]
        )

    def w_swap(i):
        return remote(
            (wg_hbm, wu_hbm)[i].at[:, units(other)], w_x.at[:, i * half:(i + 1) * half],
            ws_sem.at[i], wr_sem.at[i], {"tp": other},
        )

    def t_copy(d):
        return remote(tbl_out.at[z_at(d)], tbl.at[z], ts_sem.at[d - 1], tr_sem.at[d - 1], z_dev(d))

    def z_copy(c, d):
        return remote(
            tok.at[c, zrows(z)], tok.at[c, zrows(z)],
            zs_sem.at[d - 1, c], zr_sem.at[d - 1, c], z_dev(d),
        )

    def p_copy(c, k):
        return remote(
            send.at[c, k - 1], rows.at[c, prows(p)],
            ps_sem.at[k - 1, c], pr_sem.at[k - 1, c], p_dev(k),
        )

    def x_copy(c):
        return remote(rows.at[c], rows_x.at[c], xs_sem.at[c], xr_sem.at[c], {"tp": other})

    def h_copy(m):
        here = hid.at[t, m * R:(m + 1) * R]
        return remote(here, here, hs_sem.at[m], hr_sem.at[m], {"tp": other})

    def b_copy(c, k):
        return remote(
            outs.at[c, k - 1], ret.at[c, prows(p)],
            bs_sem.at[k - 1, c], br_sem.at[k - 1, c], p_dev(k),
        )

    def c_copy(c, d):
        return remote(
            part.at[c, zrows(z_at(d))], zin.at[c, d - 1],
            cs_sem.at[d - 1, c], cr_sem.at[d - 1, c], z_dev(d),
        )

    barrier = pltpu.get_barrier_semaphore()
    for d in range(1, line):
        pl.semaphore_signal(barrier, inc=1, device_id=z_dev(d), device_id_type=MESH)
    for k in range(1, plane):
        pl.semaphore_signal(barrier, inc=1, device_id=p_dev(k), device_id_type=MESH)
    pl.semaphore_signal(barrier, inc=1, device_id={"tp": other}, device_id_type=MESH)

    for c in range(nc):
        tok_load(c).start()
    for i in range(2):
        w_load(i).start()
    for c in range(nc):
        wd_load(c).start()

    lane = lax.broadcasted_iota(jnp.int32, (T, 128), 1)
    code = code_ref[...]
    levels = levels_ref[...].astype(F32)
    weights = levels / jnp.sum(levels, axis=1, keepdims=True)
    named = jnp.zeros((T, 128), F32)
    share = jnp.zeros((T, 128), F32)
    for k in range(top):
        at = code[:, k:k + 1]
        named = jnp.where(lane == at, 1.0, named)
        share = jnp.where(lane == at + plane, weights[:, k:k + 1], share)
    before = lax.broadcasted_iota(jnp.int32, (T, T), 0) > lax.broadcasted_iota(jnp.int32, (T, T), 1)
    count = jnp.dot(
        jnp.where(before, 1.0, 0.0).astype(BF16), named.astype(BF16), preferred_element_type=F32
    )
    slots = jnp.where(named > 0.0, count, ABSENT)
    both = jnp.where((lane & (2 * plane - 1)) < plane, slots, share).T
    for i in range(line):
        tbl_out[i] = both[i * 2 * plane:(i + 1) * 2 * plane]
    tbl[z] = tbl_out[z]

    pl.semaphore_wait(barrier, line + plane - 1)
    for d in range(1, line):
        t_copy(d).start()
    for c in range(nc):
        tok_load(c).wait()
        for d in range(1, line):
            z_copy(c, d).start()
    for i in range(2):
        w_swap(i).start()

    for d in range(1, line):
        t_copy(d).wait_recv()
    row_id = lax.broadcasted_iota(jnp.int32, (R, T), 0).astype(F32)
    for q in range(plane):
        for s in range(line):
            at = tbl[s, q:q + 1, :] + float(s * cap)
            pick[q, :, s * T:(s + 1) * T] = jnp.where(row_id == at, 1.0, 0.0).astype(BF16)

    def dispatch(c, carry):
        @pl.when(c < nc)
        def _():
            for d in range(1, line):
                z_copy(c, d).wait_recv()
            for k in range(1, plane):
                send[c, k - 1] = jnp.dot(
                    pick[p_at(k)], tok[c], preferred_element_type=F32
                ).astype(BF16)
                p_copy(c, k).start()
            rows[c, prows(p)] = jnp.dot(pick[p], tok[c], preferred_element_type=F32).astype(BF16)

        @pl.when(c == 0)
        def _():
            acc[...] = jnp.zeros_like(acc)
            slot_id = lax.broadcasted_iota(jnp.int32, (T, plane * R), 1).astype(F32)
            for s in range(line):
                columns = tbl[s].T
                high = jnp.zeros((T, plane * R), F32)
                low = jnp.zeros((T, plane * R), F32)
                for q in range(plane):
                    here = slot_id == columns[:, q:q + 1] + float(q * R + s * cap)
                    w = columns[:, plane + q:plane + q + 1]
                    w_high = w.astype(BF16).astype(F32)
                    high = jnp.where(here, w_high, high)
                    low = jnp.where(here, w - w_high, low)
                mix[0, s * T:(s + 1) * T, :] = high.astype(BF16)
                mix[1, s * T:(s + 1) * T, :] = low.astype(BF16)

        @pl.when(c == 2)
        def _():
            for i in range(2):
                w_load(i).wait()
                w_swap(i).wait()

        @pl.when((c >= 1) & (c <= nc))
        def _():
            for k in range(1, plane):
                p_copy(c - 1, k).wait_recv()
            x_copy(c - 1).start()

        @pl.when(c >= 2)
        def _():
            b = c - 2
            x_copy(b).wait_recv()
            at = pl.ds(pl.multiple_of(b * fc, fc), fc)

            def tile(m, carry):
                r = prows(m)
                acc[r] += jnp.dot(
                    rows[b, r], w_own[at], preferred_element_type=F32
                ) + jnp.dot(rows_x[b, r], w_x[at], preferred_element_type=F32)
                return carry

            lax.fori_loop(0, plane, tile, 0)

        return carry

    lax.fori_loop(0, nc + 2, dispatch, 0)

    for m in range(plane):
        gate = acc[m * R:(m + 1) * R, :half]
        up = acc[m * R:(m + 1) * R, half:]
        hid[t, m * R:(m + 1) * R] = (gate / (1.0 + jnp.exp(-gate)) * up).astype(BF16)
        h_copy(m).start()
    for c in range(nc):
        wd_load(c).wait()
    for m in range(plane):
        h_copy(m).wait_recv()

    def down(c, q):
        total = jnp.dot(hid[0, prows(q)], wd[c, :half], preferred_element_type=F32)
        total += jnp.dot(hid[1, prows(q)], wd[c, half:], preferred_element_type=F32)
        return total.astype(BF16)

    def combine(c, carry):
        @pl.when(c < nc)
        def _():
            for k in range(1, plane):
                outs[c, k - 1] = down(c, p_at(k))
                b_copy(c, k).start()
            ret[c, prows(p)] = down(c, p)

        @pl.when((c >= 1) & (c <= nc))
        def _():
            b = c - 1
            for k in range(1, plane):
                b_copy(b, k).wait_recv()
            total = jnp.dot(mix[0], ret[b], preferred_element_type=F32)
            total += jnp.dot(mix[1], ret[b], preferred_element_type=F32)
            part_f[...] = total
            part[b] = total.astype(BF16)
            for d in range(1, line):
                c_copy(b, d).start()
            own[b] = part_f[zrows(z)]

        @pl.when(c >= 2)
        def _():
            b = c - 2
            total = own[b]
            for d in range(1, line):
                c_copy(b, d).wait_recv()
                total += zin[b, d - 1].astype(F32)
            out_ref[:, pl.ds(pl.multiple_of(b * fc, fc), fc)] = total.astype(BF16)

        return carry

    lax.fori_loop(0, nc + 2, combine, 0)

    for d in range(1, line):
        t_copy(d).wait_send()
    for m in range(plane):
        h_copy(m).wait_send()

    def drain(c, carry):
        for d in range(1, line):
            z_copy(c, d).wait_send()
            c_copy(c, d).wait_send()
        for k in range(1, plane):
            p_copy(c, k).wait_send()
            b_copy(c, k).wait_send()
        x_copy(c).wait_send()
        return carry

    lax.fori_loop(0, nc, drain, 0)


def kernel_path(line, plane, cap, fc, tokens, routes, gate_levels, w_gate, w_up, w_down):
    T, width = tokens.shape
    units = w_gate.shape[2]
    half = units // 2
    R = line * cap
    nc = width // fc
    code = routes // plane * (2 * plane) + routes % plane
    vmem, dma = pltpu.VMEM, pltpu.SemaphoreType.DMA
    anywhere = pl.BlockSpec(memory_space=pl.ANY)
    local = pl.BlockSpec(memory_space=pltpu.VMEM)
    return pl.pallas_call(
        functools.partial(layer_kernel, line, plane, cap, fc),
        out_shape=jax.ShapeDtypeStruct((T, width), BF16),
        in_specs=[local, local, anywhere, anywhere, anywhere, anywhere],
        out_specs=local,
        scratch_shapes=[
            vmem((nc, line * T, fc), BF16),
            vmem((line, 2 * plane, T), F32),
            vmem((line, 2 * plane, T), F32),
            vmem((plane, R, line * T), BF16),
            vmem((2, line * T, plane * R), BF16),
            vmem((nc, plane - 1, R, fc), BF16),
            vmem((nc, plane * R, fc), BF16),
            vmem((nc, plane * R, fc), BF16),
            vmem((width, units), BF16),
            vmem((width, units), BF16),
            vmem((nc, units, fc), BF16),
            vmem((plane * R, units), F32),
            vmem((2, plane * R, half), BF16),
            vmem((nc, plane - 1, R, fc), BF16),
            vmem((nc, plane * R, fc), BF16),
            vmem((line * T, fc), F32),
            vmem((nc, line * T, fc), BF16),
            vmem((nc, line - 1, T, fc), BF16),
            vmem((nc, T, fc), F32),
            dma((nc,)), dma((2,)), dma((nc,)),
            dma((line - 1,)), dma((line - 1,)),
            dma((line - 1, nc)), dma((line - 1, nc)),
            dma((plane - 1, nc)), dma((plane - 1, nc)),
            dma((nc,)), dma((nc,)),
            dma((2,)), dma((2,)),
            dma((plane,)), dma((plane,)),
            dma((plane - 1, nc)), dma((plane - 1, nc)),
            dma((line - 1, nc)), dma((line - 1, nc)),
        ],
        compiler_params=pltpu.CompilerParams(
            collective_id=0, has_side_effects=True, vmem_limit_bytes=60 * 1024 * 1024
        ),
        name="expert_layer",
    )(code, gate_levels, tokens, w_gate[0], w_up[0], w_down[0])


def on_device(ep_count, tp_count, tokens, routes, gate_levels, w_gate, w_up, w_down):
    tok_rows, top_count = routes.shape
    experts_here, width, units = w_gate.shape
    cap = capacity_of(tok_rows, top_count, experts_here * ep_count)
    plane = math.isqrt(ep_count)
    line = ep_count // plane
    fc = 256
    fits = (
        tp_count == 2
        and experts_here == 1
        and plane * line == ep_count
        and plane & (plane - 1) == 0
        and plane % 4 == 0
        and line * 2 * plane <= 128
        and tok_rows == 128
        and line * cap % 16 == 0
        and width % fc == 0
        and units % 256 == 0
    )
    args = (tokens, routes, gate_levels, w_gate, w_up, w_down)
    if fits:
        return kernel_path(line, plane, cap, fc, *args)
    return general_path(*args)


def solution(mesh):
    in_specs = (
        P("ep", "tp"),
        P("ep", None),
        P("ep", None),
        P("ep", "tp", None),
        P("ep", "tp", None),
        P("ep", None, "tp"),
    )
    out_specs = P("ep", "tp")
    body = functools.partial(on_device, mesh.shape["ep"], mesh.shape["tp"])
    return jax.shard_map(
        body, mesh=mesh, in_specs=in_specs, out_specs=out_specs, check_vma=False
    )
```

```python
import functools
import math

import jax
import jax.numpy as jnp
from jax import lax
from jax.experimental import pallas as pl
from jax.experimental.pallas import tpu as pltpu
from jax.sharding import PartitionSpec as P

MESH = pl.DeviceIdType.MESH
ABSENT = -65536.0
F32 = jnp.float32
BF16 = jnp.bfloat16


def run_expert(inputs, gate_w, up_w, down_w):
    gate_part = jnp.dot(inputs, gate_w, preferred_element_type=jnp.float32)
    up_part = jnp.dot(inputs, up_w, preferred_element_type=jnp.float32)
    gate_sum, up_sum = (
        lax.psum_scatter(gate_part, "tp", scatter_dimension=1, tiled=True),
        lax.psum_scatter(up_part, "tp", scatter_dimension=1, tiled=True),
    )
    hidden = (jax.nn.silu(gate_sum) * up_sum).astype(jnp.bfloat16)
    output = jnp.dot(
        lax.all_gather(hidden, "tp", axis=1, tiled=True), down_w, preferred_element_type=jnp.float32
    )
    return output.astype(jnp.bfloat16)


def general_path(tokens, routes, gate_levels, w_gate, w_up, w_down):
    ep_count = lax.axis_size("ep")
    tok_rows, top_count = routes.shape
    experts_here = w_gate.shape[0]
    capacity = capacity_of(tok_rows, top_count, experts_here * ep_count)
    width_local = tokens.shape[1]
    slots_each = ep_count * capacity
    slots_total = experts_here * slots_each
    flat_ids = routes.reshape(-1)
    positions = jnp.arange(tok_rows * top_count, dtype=jnp.int32)
    same_expert = flat_ids[:, None] == flat_ids[None, :]
    earlier = positions[:, None] > positions[None, :]
    slot_index = jnp.sum(same_expert & earlier, axis=1)
    destination = (
        flat_ids % experts_here * ep_count + flat_ids // experts_here
    ) * capacity + slot_index
    slot_numbers = jnp.arange(slots_total, dtype=jnp.int32)
    matches = destination.reshape(tok_rows, top_count)[:, :, None] == slot_numbers[None, None, :]
    token_slots = jnp.any(matches, axis=1).astype(jnp.bfloat16)
    outgoing = jnp.einsum(
        "ts,td->sd", token_slots, tokens, preferred_element_type=jnp.float32
    ).astype(jnp.bfloat16)
    levels = gate_levels.astype(jnp.float32)
    weights = levels / jnp.sum(levels, axis=1, keepdims=True)
    weight_high = weights.astype(jnp.bfloat16).astype(jnp.float32)
    weight_low = weights - weight_high
    table_high = jnp.sum(jnp.where(matches, weight_high[:, :, None], 0.0), axis=1).astype(
        jnp.bfloat16
    )
    table_low = jnp.sum(jnp.where(matches, weight_low[:, :, None], 0.0), axis=1).astype(
        jnp.bfloat16
    )
    arrived = lax.all_to_all(
        outgoing.reshape(experts_here, ep_count, capacity, width_local),
        "ep",
        split_axis=1,
        concat_axis=1,
        tiled=True,
    )
    expert_rows = arrived.reshape(experts_here, slots_each, width_local)
    results = [run_expert(expert_rows[0], w_gate[0], w_up[0], w_down[0])]
    produced = jnp.stack(results)
    returned = lax.all_to_all(
        produced.reshape(experts_here, ep_count, capacity, width_local),
        "ep",
        split_axis=1,
        concat_axis=1,
        tiled=True,
    )
    flat_returned = returned.reshape(slots_total, width_local)
    mixed = jnp.dot(table_high, flat_returned, preferred_element_type=jnp.float32)
    mixed = mixed + jnp.dot(table_low, flat_returned, preferred_element_type=jnp.float32)
    return mixed.astype(jnp.bfloat16)


def capacity_of(tok_rows, top_count, experts):
    return min(tok_rows, max(2, 9 * tok_rows * top_count // (8 * experts)))


def layer_kernel(
    line, plane, cap, fc,
    routes_ref, levels_ref, tokens_hbm, wg_hbm, wu_hbm, wd_hbm, out_ref,
    tok, tbl_out, tbl, pick, mix, send, rows, rows_x, w_own, w_x, wd, acc, hid,
    outs, ret, part_f, part, zin, own,
    tok_sem, w_sem, wd_sem, ts_sem, tr_sem, zs_sem, zr_sem, ps_sem, pr_sem,
    xs_sem, xr_sem, ws_sem, wr_sem, hs_sem, hr_sem, bs_sem, br_sem, cs_sem, cr_sem,
):
    me = lax.axis_index("ep")
    t = lax.axis_index("tp")
    other = 1 - t
    z, p = me // plane, me % plane
    top, T = levels_ref.shape
    G = line // 2
    R = G * cap
    nc = tok.shape[1]
    half = wg_hbm.shape[1] // 2
    mine = lax.rem(z, G)
    near = [(0, d) for d in range(1, G)]
    far = [(1, d) for d in range(G)]
    peers = {gd: i for i, gd in enumerate(near + far)}

    def z_at(g, d):
        return lax.rem(z // G + g, 2) * G + lax.rem(mine + d, G)

    def z_dev(g, d):
        return {"ep": z_at(g, d) * plane + p}

    def p_at(k):
        return lax.rem(p + k, plane)

    def p_dev(k):
        return {"ep": z * plane + p_at(k)}

    def remote(src, dst, s, r, dev):
        return pltpu.make_async_remote_copy(
            src_ref=src, dst_ref=dst, send_sem=s, recv_sem=r, device_id=dev, device_id_type=MESH
        )

    def zrows(i):
        return pl.ds(pl.multiple_of(i * T, T), T)

    def prows(i):
        return pl.ds(pl.multiple_of(i * R, 16), R)

    def units(i):
        return pl.ds(pl.multiple_of(i * half, 128), half)

    def tok_load(c):
        return pltpu.make_async_copy(
            tokens_hbm.at[:, pl.ds(pl.multiple_of(c * fc, 128), fc)],
            tok.at[0, c, zrows(mine)], tok_sem.at[c],
        )

    def wd_load(c):
        return pltpu.make_async_copy(
            wd_hbm.at[:, pl.ds(pl.multiple_of(c * fc, 128), fc)], wd.at[c], wd_sem.at[c]
        )

    def w_load(i):
        return pltpu.make_async_copy(
            (wg_hbm, wu_hbm)[i].at[:, units(t)], w_own.at[:, i * half:(i + 1) * half], w_sem.at[i]
        )

    def w_swap(i):
        return remote(
            (wg_hbm, wu_hbm)[i].at[:, units(other)], w_x.at[:, i * half:(i + 1) * half],
            ws_sem.at[i], wr_sem.at[i], {"tp": other},
        )

    def t_copy(g, d):
        i = peers[g, d]
        return remote(
            tbl_out.at[z_at(g, d)], tbl.at[g, mine], ts_sem.at[i], tr_sem.at[i], z_dev(g, d)
        )

    def z_copy(c, g, d):
        i = peers[g, d]
        return remote(
            tok.at[0, c, zrows(mine)], tok.at[g, c, zrows(mine)],
            zs_sem.at[i, c], zr_sem.at[i, c], z_dev(g, d),
        )

    def p_copy(g, c, k):
        return remote(
            send.at[g, c, k - 1], rows.at[g, c, prows(p)],
            ps_sem.at[g, k - 1, c], pr_sem.at[g, k - 1, c], p_dev(k),
        )

    def x_copy(g, c):
        return remote(
            rows.at[g, c], rows_x.at[g, c], xs_sem.at[g, c], xr_sem.at[g, c], {"tp": other}
        )

    def h_copy(g, m):
        here = hid.at[g, t, m * R:(m + 1) * R]
        return remote(here, here, hs_sem.at[g, m], hr_sem.at[g, m], {"tp": other})

    def b_copy(g, c, k):
        return remote(
            outs.at[g, c, k - 1], ret.at[g, c, prows(p)],
            bs_sem.at[g, k - 1, c], br_sem.at[g, k - 1, c], p_dev(k),
        )

    def c_copy(c, g, d):
        i = peers[g, d]
        return remote(
            part.at[g, c, zrows(lax.rem(mine + d, G))], zin.at[c, i],
            cs_sem.at[i, c], cr_sem.at[i, c], z_dev(g, d),
        )

    barrier = pltpu.get_barrier_semaphore()
    for g, d in peers:
        pl.semaphore_signal(barrier, inc=1, device_id=z_dev(g, d), device_id_type=MESH)
    for k in range(1, plane):
        pl.semaphore_signal(barrier, inc=1, device_id=p_dev(k), device_id_type=MESH)
    pl.semaphore_signal(barrier, inc=1, device_id={"tp": other}, device_id_type=MESH)

    for c in range(nc):
        tok_load(c).start()
    for i in range(2):
        w_load(i).start()
    for c in range(nc):
        wd_load(c).start()

    height = line * 2 * plane
    row = lax.broadcasted_iota(jnp.int32, (height, T), 0)
    expert = (row >> (2 * plane).bit_length() - 1) * plane + (row & (plane - 1))
    routes = routes_ref[...]
    levels = levels_ref[...].astype(F32)
    weights = levels / jnp.sum(levels, axis=0, keepdims=True)
    named = jnp.zeros((height, T), F32)
    share = jnp.zeros((height, T), F32)
    for k in range(top):
        at = expert == routes[k:k + 1, :]
        named = jnp.where(at, 1.0, named)
        share = jnp.where(at, weights[k:k + 1, :], share)
    before = lax.broadcasted_iota(jnp.int32, (T, T), 0) < lax.broadcasted_iota(jnp.int32, (T, T), 1)
    count = jnp.dot(
        named.astype(BF16), jnp.where(before, 1.0, 0.0).astype(BF16), preferred_element_type=F32
    )
    slots = jnp.where(named > 0.0, count, ABSENT)
    both = jnp.where((row & (2 * plane - 1)) < plane, slots, share)
    for i in range(line):
        tbl_out[i] = both[i * 2 * plane:(i + 1) * 2 * plane]
    tbl[0, mine] = tbl_out[z]

    pl.semaphore_wait(barrier, line + plane - 1)
    for g, d in peers:
        t_copy(g, d).start()
    for c in range(nc):
        tok_load(c).wait()
        for g, d in near:
            z_copy(c, g, d).start()
    for c in range(nc):
        for g, d in far:
            z_copy(c, g, d).start()
    for i in range(2):
        w_swap(i).start()

    for g, d in peers:
        t_copy(g, d).wait_recv()
    row_id = lax.broadcasted_iota(jnp.int32, (R, T), 0).astype(F32)
    for g in range(2):
        for q in range(plane):
            for s in range(G):
                at = tbl[g, s, q:q + 1, :] + float(s * cap)
                pick[g, q, :, s * T:(s + 1) * T] = jnp.where(row_id == at, 1.0, 0.0).astype(BF16)

    def select(g, c):
        for k in range(1, plane):
            send[g, c, k - 1] = jnp.dot(
                pick[g, p_at(k)], tok[g, c], preferred_element_type=F32
            ).astype(BF16)
            p_copy(g, c, k).start()
        rows[g, c, prows(p)] = jnp.dot(
            pick[g, p], tok[g, c], preferred_element_type=F32
        ).astype(BF16)

    def forward(g, c):
        for k in range(1, plane):
            p_copy(g, c, k).wait_recv()
        x_copy(g, c).start()

    def gate_up(g, c):
        x_copy(g, c).wait_recv()
        at = pl.ds(pl.multiple_of(c * fc, fc), fc)

        def tile(m, carry):
            r = pl.ds(pl.multiple_of(m * 2 * R, 16), 2 * R)
            acc[g, r] += jnp.dot(
                rows[g, c, r], w_own[at], preferred_element_type=F32
            ) + jnp.dot(rows_x[g, c, r], w_x[at], preferred_element_type=F32)
            return carry

        lax.fori_loop(0, plane // 2, tile, 0)

    def activate(g):
        for m in range(plane):
            gate = acc[g, m * R:(m + 1) * R, :half]
            up = acc[g, m * R:(m + 1) * R, half:]
            hid[g, t, m * R:(m + 1) * R] = (gate / (1.0 + jnp.exp(-gate)) * up).astype(BF16)
            h_copy(g, m).start()

    def down(g, c, q):
        total = jnp.dot(hid[g, 0, prows(q)], wd[c, :half], preferred_element_type=F32)
        total += jnp.dot(hid[g, 1, prows(q)], wd[c, half:], preferred_element_type=F32)
        return total.astype(BF16)

    def give_back(g, c):
        for k in range(1, plane):
            outs[g, c, k - 1] = down(g, c, p_at(k))
            b_copy(g, c, k).start()
        ret[g, c, prows(p)] = down(g, c, p)

    def weigh(g, c):
        for k in range(1, plane):
            b_copy(g, c, k).wait_recv()
        total = jnp.dot(mix[g, 0], ret[g, c], preferred_element_type=F32)
        total += jnp.dot(mix[g, 1], ret[g, c], preferred_element_type=F32)
        part[g, c] = total.astype(BF16)
        for h, d in near if g == 0 else far:
            c_copy(c, h, d).start()
        if g == 0:
            part_f[...] = total
            own[c] = part_f[zrows(mine)]

    def first(c, carry):
        for g, d in near:
            z_copy(c, g, d).wait_recv()
        select(0, c)
        return carry

    lax.fori_loop(0, nc, first, 0)

    acc[...] = jnp.zeros_like(acc)
    slot_id = lax.broadcasted_iota(jnp.int32, (T, plane * R), 1).astype(F32)
    for g in range(2):
        for s in range(G):
            columns = tbl[g, s].T
            high = jnp.zeros((T, plane * R), F32)
            low = jnp.zeros((T, plane * R), F32)
            for q in range(plane):
                here = slot_id == columns[:, q:q + 1] + float(q * R + s * cap)
                w = columns[:, plane + q:plane + q + 1]
                w_high = w.astype(BF16).astype(F32)
                high = jnp.where(here, w_high, high)
                low = jnp.where(here, w - w_high, low)
            mix[g, 0, s * T:(s + 1) * T, :] = high.astype(BF16)
            mix[g, 1, s * T:(s + 1) * T, :] = low.astype(BF16)
    for i in range(2):
        w_load(i).wait()
        w_swap(i).wait()
    for c in range(nc):
        wd_load(c).wait()

    lag = 3
    early = min(3, nc)

    def dispatch(c, carry):
        @pl.when(c < nc)
        def _():
            for g, d in far:
                z_copy(c, g, d).wait_recv()
            select(1, c)
            forward(0, c)

        @pl.when((c >= 1) & (c <= nc))
        def _():
            gate_up(0, c - 1)

        @pl.when(c == nc)
        def _():
            activate(0)

        @pl.when((c >= lag) & (c < nc + lag))
        def _():
            forward(1, c - lag)

        @pl.when(c == nc + 1)
        def _():
            for m in range(plane):
                h_copy(0, m).wait_recv()

        @pl.when((c > nc) & (c <= nc + early))
        def _():
            give_back(0, c - nc - 1)

        @pl.when(c > lag)
        def _():
            gate_up(1, c - lag - 1)

        return carry

    lax.fori_loop(0, nc + lag + 1, dispatch, 0)

    activate(1)
    for m in range(plane):
        h_copy(1, m).wait_recv()

    def back_far(c, carry):
        give_back(1, c)

        @pl.when(c < early)
        def _():
            weigh(0, c)

        @pl.when(c >= 2)
        def _():
            weigh(1, c - 2)

        return carry

    lax.fori_loop(0, nc, back_far, 0)

    def back_near(j, carry):
        @pl.when(j < nc - early)
        def _():
            give_back(0, early + j)

        @pl.when(j < 2)
        def _():
            weigh(1, nc - 2 + j)

        @pl.when(j >= 2)
        def _():
            weigh(0, early + j - 2)

        return carry

    lax.fori_loop(0, nc - early + 2, back_near, 0)

    def finish(c, carry):
        total = own[c]
        for (g, d), i in peers.items():
            c_copy(c, g, d).wait_recv()
            total += zin[c, i].astype(F32)
        out_ref[:, pl.ds(pl.multiple_of(c * fc, fc), fc)] = total.astype(BF16)
        return carry

    lax.fori_loop(0, nc, finish, 0)

    for g, d in peers:
        t_copy(g, d).wait_send()
    for g in range(2):
        for m in range(plane):
            h_copy(g, m).wait_send()

    def drain(c, carry):
        for g, d in peers:
            z_copy(c, g, d).wait_send()
            c_copy(c, g, d).wait_send()
        for g in range(2):
            for k in range(1, plane):
                p_copy(g, c, k).wait_send()
                b_copy(g, c, k).wait_send()
            x_copy(g, c).wait_send()
        return carry

    lax.fori_loop(0, nc, drain, 0)


def kernel_path(line, plane, cap, fc, tokens, routes, gate_levels, w_gate, w_up, w_down):
    T, width = tokens.shape
    units = w_gate.shape[2]
    half = units // 2
    G = line // 2
    R = G * cap
    nc = width // fc
    vmem, dma = pltpu.VMEM, pltpu.SemaphoreType.DMA
    anywhere = pl.BlockSpec(memory_space=pl.ANY)
    local = pl.BlockSpec(memory_space=pltpu.VMEM)
    return pl.pallas_call(
        functools.partial(layer_kernel, line, plane, cap, fc),
        out_shape=jax.ShapeDtypeStruct((T, width), BF16),
        in_specs=[local, local, anywhere, anywhere, anywhere, anywhere],
        out_specs=local,
        scratch_shapes=[
            vmem((2, nc, G * T, fc), BF16),
            vmem((line, 2 * plane, T), F32),
            vmem((2, G, 2 * plane, T), F32),
            vmem((2, plane, R, G * T), BF16),
            vmem((2, 2, G * T, plane * R), BF16),
            vmem((2, nc, plane - 1, R, fc), BF16),
            vmem((2, nc, plane * R, fc), BF16),
            vmem((2, nc, plane * R, fc), BF16),
            vmem((width, units), BF16),
            vmem((width, units), BF16),
            vmem((nc, units, fc), BF16),
            vmem((2, plane * R, units), F32),
            vmem((2, 2, plane * R, half), BF16),
            vmem((2, nc, plane - 1, R, fc), BF16),
            vmem((2, nc, plane * R, fc), BF16),
            vmem((G * T, fc), F32),
            vmem((2, nc, G * T, fc), BF16),
            vmem((nc, line - 1, T, fc), BF16),
            vmem((nc, T, fc), F32),
            dma((nc,)), dma((2,)), dma((nc,)),
            dma((line - 1,)), dma((line - 1,)),
            dma((line - 1, nc)), dma((line - 1, nc)),
            dma((2, plane - 1, nc)), dma((2, plane - 1, nc)),
            dma((2, nc)), dma((2, nc)),
            dma((2,)), dma((2,)),
            dma((2, plane)), dma((2, plane)),
            dma((2, plane - 1, nc)), dma((2, plane - 1, nc)),
            dma((line - 1, nc)), dma((line - 1, nc)),
        ],
        compiler_params=pltpu.CompilerParams(
            collective_id=0, has_side_effects=True, vmem_limit_bytes=60 * 1024 * 1024
        ),
        name="expert_layer",
    )(routes.T, gate_levels.T, tokens, w_gate[0], w_up[0], w_down[0])


def on_device(ep_count, tp_count, tokens, routes, gate_levels, w_gate, w_up, w_down):
    tok_rows, top_count = routes.shape
    experts_here, width, units = w_gate.shape
    cap = capacity_of(tok_rows, top_count, experts_here * ep_count)
    plane = math.isqrt(ep_count)
    line = ep_count // plane
    fc = 256
    fits = (
        tp_count == 2
        and experts_here == 1
        and plane * line == ep_count
        and plane & (plane - 1) == 0
        and plane % 4 == 0
        and line * 2 * plane <= 128
        and tok_rows == 128
        and line % 2 == 0
        and line * cap % 32 == 0
        and width // fc >= 3
        and width % fc == 0
        and units % 256 == 0
    )
    args = (tokens, routes, gate_levels, w_gate, w_up, w_down)
    if fits:
        return kernel_path(line, plane, cap, fc, *args)
    return general_path(*args)


def solution(mesh):
    in_specs = (
        P("ep", "tp"),
        P("ep", None),
        P("ep", None),
        P("ep", "tp", None),
        P("ep", "tp", None),
        P("ep", None, "tp"),
    )
    out_specs = P("ep", "tp")
    body = functools.partial(on_device, mesh.shape["ep"], mesh.shape["tp"])
    return jax.shard_map(
        body, mesh=mesh, in_specs=in_specs, out_specs=out_specs, check_vma=False
    )
```

```python
import functools
import math

import jax
import jax.numpy as jnp
from jax import lax
from jax.experimental import pallas as pl
from jax.experimental.pallas import tpu as pltpu
from jax.sharding import PartitionSpec as P

MESH = pl.DeviceIdType.MESH
ABSENT = -65536.0
F32 = jnp.float32
BF16 = jnp.bfloat16


def run_expert(inputs, gate_w, up_w, down_w):
    gate_part = jnp.dot(inputs, gate_w, preferred_element_type=jnp.float32)
    up_part = jnp.dot(inputs, up_w, preferred_element_type=jnp.float32)
    gate_sum, up_sum = (
        lax.psum_scatter(gate_part, "tp", scatter_dimension=1, tiled=True),
        lax.psum_scatter(up_part, "tp", scatter_dimension=1, tiled=True),
    )
    hidden = (jax.nn.silu(gate_sum) * up_sum).astype(jnp.bfloat16)
    output = jnp.dot(
        lax.all_gather(hidden, "tp", axis=1, tiled=True), down_w, preferred_element_type=jnp.float32
    )
    return output.astype(jnp.bfloat16)


def general_path(tokens, routes, gate_levels, w_gate, w_up, w_down):
    ep_count = lax.axis_size("ep")
    tok_rows, top_count = routes.shape
    experts_here = w_gate.shape[0]
    capacity = capacity_of(tok_rows, top_count, experts_here * ep_count)
    width_local = tokens.shape[1]
    slots_each = ep_count * capacity
    slots_total = experts_here * slots_each
    flat_ids = routes.reshape(-1)
    positions = jnp.arange(tok_rows * top_count, dtype=jnp.int32)
    same_expert = flat_ids[:, None] == flat_ids[None, :]
    earlier = positions[:, None] > positions[None, :]
    slot_index = jnp.sum(same_expert & earlier, axis=1)
    destination = (
        flat_ids % experts_here * ep_count + flat_ids // experts_here
    ) * capacity + slot_index
    slot_numbers = jnp.arange(slots_total, dtype=jnp.int32)
    matches = destination.reshape(tok_rows, top_count)[:, :, None] == slot_numbers[None, None, :]
    token_slots = jnp.any(matches, axis=1).astype(jnp.bfloat16)
    outgoing = jnp.einsum(
        "ts,td->sd", token_slots, tokens, preferred_element_type=jnp.float32
    ).astype(jnp.bfloat16)
    levels = gate_levels.astype(jnp.float32)
    weights = levels / jnp.sum(levels, axis=1, keepdims=True)
    weight_high = weights.astype(jnp.bfloat16).astype(jnp.float32)
    weight_low = weights - weight_high
    table_high = jnp.sum(jnp.where(matches, weight_high[:, :, None], 0.0), axis=1).astype(
        jnp.bfloat16
    )
    table_low = jnp.sum(jnp.where(matches, weight_low[:, :, None], 0.0), axis=1).astype(
        jnp.bfloat16
    )
    arrived = lax.all_to_all(
        outgoing.reshape(experts_here, ep_count, capacity, width_local),
        "ep",
        split_axis=1,
        concat_axis=1,
        tiled=True,
    )
    expert_rows = arrived.reshape(experts_here, slots_each, width_local)
    results = [run_expert(expert_rows[0], w_gate[0], w_up[0], w_down[0])]
    produced = jnp.stack(results)
    returned = lax.all_to_all(
        produced.reshape(experts_here, ep_count, capacity, width_local),
        "ep",
        split_axis=1,
        concat_axis=1,
        tiled=True,
    )
    flat_returned = returned.reshape(slots_total, width_local)
    mixed = jnp.dot(table_high, flat_returned, preferred_element_type=jnp.float32)
    mixed = mixed + jnp.dot(table_low, flat_returned, preferred_element_type=jnp.float32)
    return mixed.astype(jnp.bfloat16)


def capacity_of(tok_rows, top_count, experts):
    return min(tok_rows, max(2, 9 * tok_rows * top_count // (8 * experts)))


def layer_kernel(
    line, plane, cap, fc,
    routes_ref, levels_ref, tokens_hbm, wg_hbm, wu_hbm, wd_hbm, out_ref,
    tok, tbl_out, tbl, pick, mix, send, rows, rows_x, w_own, w_x, wd, acc, hid,
    outs, ret, part_f, part, zin, own,
    tok_sem, w_sem, wd_sem, ts_sem, tr_sem, zs_sem, zr_sem, ps_sem, pr_sem,
    xs_sem, xr_sem, ws_sem, wr_sem, hs_sem, hr_sem, bs_sem, br_sem, cs_sem, cr_sem,
):
    me = lax.axis_index("ep")
    t = lax.axis_index("tp")
    other = 1 - t
    z, p = me // plane, me % plane
    top, T = levels_ref.shape
    G = line // 2
    R = G * cap
    nc = tok.shape[1]
    half = wg_hbm.shape[1] // 2
    mine = lax.rem(z, G)
    near = [(0, d) for d in range(1, G)]
    far = [(1, d) for d in range(G)]
    peers = {gd: i for i, gd in enumerate(near + far)}

    def z_at(g, d):
        return lax.rem(z // G + g, 2) * G + lax.rem(mine + d, G)

    def z_dev(g, d):
        return {"ep": z_at(g, d) * plane + p}

    def p_at(k):
        return lax.rem(p + k, plane)

    def p_dev(k):
        return {"ep": z * plane + p_at(k)}

    def remote(src, dst, s, r, dev):
        return pltpu.make_async_remote_copy(
            src_ref=src, dst_ref=dst, send_sem=s, recv_sem=r, device_id=dev, device_id_type=MESH
        )

    def zrows(i):
        return pl.ds(pl.multiple_of(i * T, T), T)

    def prows(i):
        return pl.ds(pl.multiple_of(i * R, 16), R)

    def units(i):
        return pl.ds(pl.multiple_of(i * half, 128), half)

    def tok_load(c):
        return pltpu.make_async_copy(
            tokens_hbm.at[:, pl.ds(pl.multiple_of(c * fc, 128), fc)],
            tok.at[0, c, zrows(mine)], tok_sem.at[c],
        )

    def wd_load(c):
        return pltpu.make_async_copy(
            wd_hbm.at[:, pl.ds(pl.multiple_of(c * fc, 128), fc)], wd.at[c], wd_sem.at[c]
        )

    def w_load(i):
        return pltpu.make_async_copy(
            (wg_hbm, wu_hbm)[i].at[:, units(t)], w_own.at[:, i * half:(i + 1) * half], w_sem.at[i]
        )

    def w_swap(i):
        return remote(
            (wg_hbm, wu_hbm)[i].at[:, units(other)], w_x.at[:, i * half:(i + 1) * half],
            ws_sem.at[i], wr_sem.at[i], {"tp": other},
        )

    def t_copy(g, d):
        i = peers[g, d]
        return remote(
            tbl_out.at[z_at(g, d)], tbl.at[g, mine], ts_sem.at[i], tr_sem.at[i], z_dev(g, d)
        )

    def z_copy(c, g, d):
        i = peers[g, d]
        return remote(
            tok.at[0, c, zrows(mine)], tok.at[g, c, zrows(mine)],
            zs_sem.at[i, c], zr_sem.at[i, c], z_dev(g, d),
        )

    def p_copy(g, c, k):
        return remote(
            send.at[g, c, k - 1], rows.at[g, c, prows(p)],
            ps_sem.at[g, k - 1, c], pr_sem.at[g, k - 1, c], p_dev(k),
        )

    def x_copy(g, c):
        return remote(
            rows.at[g, c], rows_x.at[g, c], xs_sem.at[g, c], xr_sem.at[g, c], {"tp": other}
        )

    def h_copy(g, m):
        here = hid.at[g, t, m * R:(m + 1) * R]
        return remote(here, here, hs_sem.at[g, m], hr_sem.at[g, m], {"tp": other})

    def b_copy(g, c, k):
        return remote(
            outs.at[g, c, k - 1], ret.at[g, c, prows(p)],
            bs_sem.at[g, k - 1, c], br_sem.at[g, k - 1, c], p_dev(k),
        )

    def c_copy(c, g, d):
        i = peers[g, d]
        return remote(
            part.at[g, c, zrows(lax.rem(mine + d, G))], zin.at[c, i],
            cs_sem.at[i, c], cr_sem.at[i, c], z_dev(g, d),
        )

    barrier = pltpu.get_barrier_semaphore()
    for g, d in peers:
        pl.semaphore_signal(barrier, inc=1, device_id=z_dev(g, d), device_id_type=MESH)
    for k in range(1, plane):
        pl.semaphore_signal(barrier, inc=1, device_id=p_dev(k), device_id_type=MESH)
    pl.semaphore_signal(barrier, inc=1, device_id={"tp": other}, device_id_type=MESH)

    for c in range(nc):
        tok_load(c).start()
    for i in range(2):
        w_load(i).start()
    for c in range(nc):
        wd_load(c).start()

    height = line * 2 * plane
    row = lax.broadcasted_iota(jnp.int32, (height, T), 0)
    expert = (row >> (2 * plane).bit_length() - 1) * plane + (row & (plane - 1))
    routes = routes_ref[...]
    levels = levels_ref[...].astype(F32)
    weights = levels / jnp.sum(levels, axis=0, keepdims=True)
    named = jnp.zeros((height, T), F32)
    share = jnp.zeros((height, T), F32)
    for k in range(top):
        at = expert == routes[k:k + 1, :]
        named = jnp.where(at, 1.0, named)
        share = jnp.where(at, weights[k:k + 1, :], share)
    before = lax.broadcasted_iota(jnp.int32, (T, T), 0) < lax.broadcasted_iota(jnp.int32, (T, T), 1)
    count = jnp.dot(
        named.astype(BF16), jnp.where(before, 1.0, 0.0).astype(BF16), preferred_element_type=F32
    )
    slots = jnp.where(named > 0.0, count, ABSENT)
    both = jnp.where((row & (2 * plane - 1)) < plane, slots, share)
    for i in range(line):
        tbl_out[i] = both[i * 2 * plane:(i + 1) * 2 * plane]
    tbl[0, mine] = tbl_out[z]

    pl.semaphore_wait(barrier, line + plane - 1)
    for g, d in peers:
        t_copy(g, d).start()
    for c in range(nc):
        tok_load(c).wait()
        for g, d in near:
            z_copy(c, g, d).start()
    for c in range(nc):
        for g, d in far:
            z_copy(c, g, d).start()
    for i in range(2):
        w_swap(i).start()

    for g, d in peers:
        t_copy(g, d).wait_recv()
    row_id = lax.broadcasted_iota(jnp.int32, (R, T), 0).astype(F32)
    for g in range(2):
        for q in range(plane):
            for s in range(G):
                at = tbl[g, s, q:q + 1, :] + float(s * cap)
                pick[g, q, :, s * T:(s + 1) * T] = jnp.where(row_id == at, 1.0, 0.0).astype(BF16)

    def select(g, c):
        for k in range(1, plane):
            send[g, c, k - 1] = jnp.dot(
                pick[g, p_at(k)], tok[g, c], preferred_element_type=F32
            ).astype(BF16)
            p_copy(g, c, k).start()
        rows[g, c, prows(p)] = jnp.dot(
            pick[g, p], tok[g, c], preferred_element_type=F32
        ).astype(BF16)

    def forward(g, c):
        for k in range(1, plane):
            p_copy(g, c, k).wait_recv()
        x_copy(g, c).start()

    def gate_up(g, c):
        x_copy(g, c).wait_recv()
        at = pl.ds(pl.multiple_of(c * fc, fc), fc)

        def tile(m, carry):
            r = pl.ds(pl.multiple_of(m * 2 * R, 16), 2 * R)
            acc[g, r] += jnp.dot(
                rows[g, c, r], w_own[at], preferred_element_type=F32
            ) + jnp.dot(rows_x[g, c, r], w_x[at], preferred_element_type=F32)
            return carry

        lax.fori_loop(0, plane // 2, tile, 0)

    def activate(g):
        for m in range(plane):
            gate = acc[g, m * R:(m + 1) * R, :half]
            up = acc[g, m * R:(m + 1) * R, half:]
            hid[g, t, m * R:(m + 1) * R] = (gate / (1.0 + jnp.exp(-gate)) * up).astype(BF16)
            h_copy(g, m).start()

    def down(g, c, q):
        total = jnp.dot(hid[g, 0, prows(q)], wd[c, :half], preferred_element_type=F32)
        total += jnp.dot(hid[g, 1, prows(q)], wd[c, half:], preferred_element_type=F32)
        return total.astype(BF16)

    def give_back(g, c):
        for k in range(1, plane):
            outs[g, c, k - 1] = down(g, c, p_at(k))
            b_copy(g, c, k).start()
        ret[g, c, prows(p)] = down(g, c, p)

    def weigh(g, c):
        for k in range(1, plane):
            b_copy(g, c, k).wait_recv()
        total = jnp.dot(mix[g, 0], ret[g, c], preferred_element_type=F32)
        total += jnp.dot(mix[g, 1], ret[g, c], preferred_element_type=F32)
        part[g, c] = total.astype(BF16)
        for h, d in near if g == 0 else far:
            c_copy(c, h, d).start()
        if g == 0:
            part_f[...] = total
            own[c] = part_f[zrows(mine)]

    def first(c, carry):
        for g, d in near:
            z_copy(c, g, d).wait_recv()
        select(0, c)
        return carry

    lax.fori_loop(0, nc, first, 0)

    acc[...] = jnp.zeros_like(acc)
    slot_id = lax.broadcasted_iota(jnp.int32, (T, plane * R), 1).astype(F32)
    for g in range(2):
        for s in range(G):
            columns = tbl[g, s].T
            high = jnp.zeros((T, plane * R), F32)
            low = jnp.zeros((T, plane * R), F32)
            for q in range(plane):
                here = slot_id == columns[:, q:q + 1] + float(q * R + s * cap)
                w = columns[:, plane + q:plane + q + 1]
                w_high = w.astype(BF16).astype(F32)
                high = jnp.where(here, w_high, high)
                low = jnp.where(here, w - w_high, low)
            mix[g, 0, s * T:(s + 1) * T, :] = high.astype(BF16)
            mix[g, 1, s * T:(s + 1) * T, :] = low.astype(BF16)
    for i in range(2):
        w_load(i).wait()
        w_swap(i).wait()
    for c in range(nc):
        wd_load(c).wait()

    lag = 3
    early = min(lag + 1, nc)

    def dispatch(c, carry):
        @pl.when(c < nc)
        def _():
            for g, d in far:
                z_copy(c, g, d).wait_recv()
            select(1, c)
            forward(0, c)

        @pl.when((c >= 1) & (c <= nc))
        def _():
            gate_up(0, c - 1)

        @pl.when(c == nc)
        def _():
            activate(0)

        @pl.when(c == nc + 1)
        def _():
            for m in range(plane):
                h_copy(0, m).wait_recv()

        @pl.when((c > nc) & (c < nc + early))
        def _():
            give_back(0, c - nc - 1)

        @pl.when((c >= lag) & (c < nc + lag))
        def _():
            forward(1, c - lag)

        @pl.when(c > lag)
        def _():
            gate_up(1, c - lag - 1)

        return carry

    lax.fori_loop(0, nc + lag + 1, dispatch, 0)

    activate(1)
    give_back(0, early - 1)
    for m in range(plane):
        h_copy(1, m).wait_recv()

    def back_far(c, carry):
        give_back(1, c)

        @pl.when(c < early)
        def _():
            weigh(0, c)

        @pl.when(c >= 2)
        def _():
            weigh(1, c - 2)

        return carry

    lax.fori_loop(0, nc, back_far, 0)

    def back_near(j, carry):
        @pl.when(j < nc - early)
        def _():
            give_back(0, early + j)

        @pl.when(j < 2)
        def _():
            weigh(1, nc - 2 + j)

        @pl.when(j >= 2)
        def _():
            weigh(0, early + j - 2)

        return carry

    lax.fori_loop(0, nc - early + 2, back_near, 0)

    def finish(c, carry):
        total = own[c]
        for (g, d), i in peers.items():
            c_copy(c, g, d).wait_recv()
            total += zin[c, i].astype(F32)
        out_ref[:, pl.ds(pl.multiple_of(c * fc, fc), fc)] = total.astype(BF16)
        return carry

    lax.fori_loop(0, nc, finish, 0)

    for g, d in peers:
        t_copy(g, d).wait_send()
    for g in range(2):
        for m in range(plane):
            h_copy(g, m).wait_send()

    def drain(c, carry):
        for g, d in peers:
            z_copy(c, g, d).wait_send()
            c_copy(c, g, d).wait_send()
        for g in range(2):
            for k in range(1, plane):
                p_copy(g, c, k).wait_send()
                b_copy(g, c, k).wait_send()
            x_copy(g, c).wait_send()
        return carry

    lax.fori_loop(0, nc, drain, 0)


def kernel_path(line, plane, cap, fc, tokens, routes, gate_levels, w_gate, w_up, w_down):
    T, width = tokens.shape
    units = w_gate.shape[2]
    half = units // 2
    G = line // 2
    R = G * cap
    nc = width // fc
    vmem, dma = pltpu.VMEM, pltpu.SemaphoreType.DMA
    anywhere = pl.BlockSpec(memory_space=pl.ANY)
    local = pl.BlockSpec(memory_space=pltpu.VMEM)
    return pl.pallas_call(
        functools.partial(layer_kernel, line, plane, cap, fc),
        out_shape=jax.ShapeDtypeStruct((T, width), BF16),
        in_specs=[local, local, anywhere, anywhere, anywhere, anywhere],
        out_specs=local,
        scratch_shapes=[
            vmem((2, nc, G * T, fc), BF16),
            vmem((line, 2 * plane, T), F32),
            vmem((2, G, 2 * plane, T), F32),
            vmem((2, plane, R, G * T), BF16),
            vmem((2, 2, G * T, plane * R), BF16),
            vmem((2, nc, plane - 1, R, fc), BF16),
            vmem((2, nc, plane * R, fc), BF16),
            vmem((2, nc, plane * R, fc), BF16),
            vmem((width, units), BF16),
            vmem((width, units), BF16),
            vmem((nc, units, fc), BF16),
            vmem((2, plane * R, units), F32),
            vmem((2, 2, plane * R, half), BF16),
            vmem((2, nc, plane - 1, R, fc), BF16),
            vmem((2, nc, plane * R, fc), BF16),
            vmem((G * T, fc), F32),
            vmem((2, nc, G * T, fc), BF16),
            vmem((nc, line - 1, T, fc), BF16),
            vmem((nc, T, fc), F32),
            dma((nc,)), dma((2,)), dma((nc,)),
            dma((line - 1,)), dma((line - 1,)),
            dma((line - 1, nc)), dma((line - 1, nc)),
            dma((2, plane - 1, nc)), dma((2, plane - 1, nc)),
            dma((2, nc)), dma((2, nc)),
            dma((2,)), dma((2,)),
            dma((2, plane)), dma((2, plane)),
            dma((2, plane - 1, nc)), dma((2, plane - 1, nc)),
            dma((line - 1, nc)), dma((line - 1, nc)),
        ],
        compiler_params=pltpu.CompilerParams(
            collective_id=0, has_side_effects=True, vmem_limit_bytes=60 * 1024 * 1024
        ),
        name="expert_layer",
    )(routes.T, gate_levels.T, tokens, w_gate[0], w_up[0], w_down[0])


def on_device(ep_count, tp_count, tokens, routes, gate_levels, w_gate, w_up, w_down):
    tok_rows, top_count = routes.shape
    experts_here, width, units = w_gate.shape
    cap = capacity_of(tok_rows, top_count, experts_here * ep_count)
    plane = math.isqrt(ep_count)
    line = ep_count // plane
    fc = 256
    fits = (
        tp_count == 2
        and experts_here == 1
        and plane * line == ep_count
        and plane & (plane - 1) == 0
        and plane % 4 == 0
        and line * 2 * plane <= 128
        and tok_rows == 128
        and line % 2 == 0
        and line * cap % 32 == 0
        and width // fc >= 4
        and width % fc == 0
        and units % 256 == 0
    )
    args = (tokens, routes, gate_levels, w_gate, w_up, w_down)
    if fits:
        return kernel_path(line, plane, cap, fc, *args)
    return general_path(*args)


def solution(mesh):
    in_specs = (
        P("ep", "tp"),
        P("ep", None),
        P("ep", None),
        P("ep", "tp", None),
        P("ep", "tp", None),
        P("ep", None, "tp"),
    )
    out_specs = P("ep", "tp")
    body = functools.partial(on_device, mesh.shape["ep"], mesh.shape["tp"])
    return jax.shard_map(
        body, mesh=mesh, in_specs=in_specs, out_specs=out_specs, check_vma=False
    )
```
